32 devices in a mesh: clip: 4 (over z), tm: 8 (over y, x, core).
Axes of the slice: x: 2, y: 2, z: 4, core: 2. Of those that a mesh axis runs over, the one named last changes fastest.
Arguments:
- tokens: bfloat16 [4, 8, 256, 2048], P('clip', 'tm'), may hold values from -16 to 16
- spatial_queries: bfloat16 [4, 8, 256, 1024], P('clip', 'tm'), may hold values from -4.5 to 4.5
- spatial_keys: bfloat16 [4, 8, 256, 1024], P('clip', 'tm'), may hold values from -4.5 to 4.5
- spatial_values: bfloat16 [4, 8, 256, 1024], P('clip', 'tm'), may hold values from -6 to 6
- spatial_proj: bfloat16 [1024, 2048], P('tm'), may hold values from -0.1875 to 0.1875
- temporal_qkv: bfloat16 [2048, 3072], P('tm'), may hold values from -0.13258252 to 0.13258252
- temporal_proj: bfloat16 [1024, 2048], P('tm'), may hold values from -0.1875 to 0.1875
- frame_mask: int32 [4, 8, 8], P('clip'), may hold values from 0 to 1, as said below
- expert_ids: int32 [4, 8, 256, 2], P('clip', 'tm'), may hold values from 0 to 31, all different within a row; in each aligned block of 256 rows (0 to 255, 256 to 511, ..., all dimensions but the last counted through in order) at most 32 rows name the same one
- gate_values: float32 [4, 8, 256, 2], P('clip', 'tm'), may hold values from 0.2 to 1
- expert_gate: bfloat16 [32, 2048, 1408], P(('clip', 'tm')), may hold values from -0.125 to 0.125
- expert_up: bfloat16 [32, 2048, 1408], P(('clip', 'tm')), may hold values from -0.125 to 0.125
- expert_down: bfloat16 [32, 1408, 2048], P(('clip', 'tm')), may hold values from -0.15625 to 0.15625
Outputs:
- layer_out: bfloat16 [4, 8, 256, 2048], P('clip', 'tm')
The draws below stay inside these ranges and needn't reach their ends.
Inputs may be any that keep to these rules, and one draw needn't show every extreme that they name: `expert_ids`: each token names 2 different experts. Among the 256 tokens of one clip and frame, no expert is named by more than 32 tokens, and in some frames one expert is named by exactly 32. frame_mask[c, i, j] is 1 where j = i and 0 where j > i.
All inputs are finite; a program needn't handle non-finite values.
Results may differ from the reference program's by a relative error of at most 0.013.
Values may be sent and summed in bfloat16 or wider, within the bound.
A program may use at most 128 MiB of HBM per device.

```python
import math
import jax
import jax.numpy as jnp
import numpy as np
from jax import lax

D = 2048
HEADS = 8
HD = 128
FF = 1408
TOP = 2
POS = 256
EXPERTS = 32
CLIPS = 4
FRAMES = 8
HH = 1024
CAP = 32


def draw_tokens(key, part):
    full_shape = (CLIPS, FRAMES, POS, D)
    values = jnp.clip(jax.random.normal(jax.random.fold_in(key, 11), full_shape, jnp.float32), -6.0, 6.0)
    return values.astype(jnp.bfloat16)


def spatial_pair(key):
    base_key = jax.random.fold_in(key, 3131)
    full_shape = (CLIPS, FRAMES, POS, HEADS, HD)
    query_side = jnp.clip(jax.random.normal(jax.random.fold_in(base_key, 1), full_shape, jnp.float32), -4.5, 4.5)
    key_side = jnp.clip(jax.random.normal(jax.random.fold_in(base_key, 2), full_shape, jnp.float32), -4.5, 4.5)
    flat_shape = (CLIPS, FRAMES, POS, HEADS * HD)
    return (query_side.reshape(flat_shape), key_side.reshape(flat_shape))


def draw_spatial_queries(key, part):
    query_side, key_side = spatial_pair(key)
    return query_side.astype(jnp.bfloat16)


def draw_spatial_keys(key, part):
    query_side, key_side = spatial_pair(key)
    return key_side.astype(jnp.bfloat16)


def draw_temporal_qkv(key, part):
    fan_scale = 1.0 / math.sqrt(D)
    full_shape = (D, 3, HEADS, HD)
    values = jax.random.normal(jax.random.fold_in(key, 21), full_shape, jnp.float32) * fan_scale
    values = jnp.clip(values, -6.0 * fan_scale, 6.0 * fan_scale)
    return values.reshape(D, 3 * HEADS * HD).astype(jnp.bfloat16)


def draw_frame_mask(key, part):
    coin_flips = jax.random.randint(jax.random.fold_in(key, 55), (CLIPS, FRAMES, FRAMES), 0, 2)
    row_index = jnp.arange(FRAMES, dtype=jnp.int32)[:, None]
    col_index = jnp.arange(FRAMES, dtype=jnp.int32)[None, :]
    diagonal = jnp.where(col_index == row_index, 1, 0)
    return jnp.where(col_index < row_index, coin_flips, diagonal[None, :, :]).astype(jnp.int32)


def block_levels(own_key, shape, cuts, low, high):
    loudness = 1.0
    for dim, shards_of in cuts:
        draws = jax.random.uniform(jax.random.fold_in(jax.random.fold_in(own_key, 6), dim), (shards_of,), jnp.float32, low / len(cuts), high / len(cuts))
        loudness = loudness * jnp.repeat(jnp.exp(draws), shape[dim] // shards_of).reshape((-1,) + (1,) * (len(shape) - 1 - dim))
    return loudness


def deal_out(key, own, number, rows, number_of, top, reach, lean):
    order = jax.random.permutation(key, number_of)
    heavy_load, common = load_shares(number_of, rows * top, reach, lean, True), load_shares(number_of, rows * top, reach, lean, False)
    places = jnp.arange(number_of)

    def named(tallies, rotation):
        used = int((tallies > 0).sum())
        fixed = max(1, used // 4)
        passed = fixed + (places - fixed + rotation * (used - fixed)) % max(1, number_of - fixed)
        return jnp.zeros((number_of,), jnp.int32).at[order[jnp.where(places < fixed, places, passed)]].set(jnp.asarray(tallies, jnp.int32))

    tallies = jnp.where(number % 4 == 0, named(heavy_load, number // 4), named(common, number - number // 4 - 1))
    mixed = jax.random.permutation(jax.random.fold_in(own, 3), number_of)
    donor, taker = mixed[0:number_of // 2 * 2:2], mixed[1:number_of // 2 * 2:2]
    slack = jnp.minimum(tallies[donor] - 1, reach - tallies[taker]) // 2
    slack = jnp.where((donor == order[0]) | (taker == order[0]) | (tallies[taker] == 0), 0, jnp.maximum(slack, 0))
    passed = jax.random.randint(jax.random.fold_in(own, 4), (number_of // 2,), 0, 1 << 20) % (slack + 1)
    tallies = tallies.at[donor].add(-passed).at[taker].add(passed)
    labels = jnp.searchsorted(jnp.cumsum(tallies), jnp.arange(rows * top), side="right").astype(jnp.int32)
    table = labels.reshape(top, rows).T
    table = table[jax.random.permutation(jax.random.fold_in(own, 1), rows)]
    rotation = jax.random.randint(jax.random.fold_in(own, 2), (rows, 1), 0, top)
    return jnp.take_along_axis(table, (jnp.arange(top)[None, :] + rotation) % top, axis=1)


def load_shares(amount, total, bound, skew, full):
    loads = [(1 << 20) // math.isqrt(grade ** skew) + 1 for grade in range(1, amount + 1)]
    largest = bound if full else min(bound, max(-(-total // amount), total * loads[0] // sum(loads)))
    least = 1 if total - largest >= amount - 1 else 0
    given, spare = [largest] + [least] * (amount - 1), total - largest - least * (amount - 1)
    while spare > 0:
        movable = [i for i in range(1, amount) if given[i] < largest] or [i for i in range(1, amount) if given[i] < bound]
        whole, left = sum([loads[i] for i in movable]), spare
        for i in movable:
            more = min(bound - given[i], max(1, left * loads[i] // whole), spare)
            given[i] = given[i] + more
            spare = spare - more
    return np.array(given)


def gaussian(key, shape, deviation, reach, cuts=(), kind=jnp.bfloat16):
    entries = jax.random.normal(key, shape, jnp.float32) * deviation
    if len(cuts) > 0:
        entries = block_levels(key, shape, cuts, -0.22, 0.18) * entries
    return jnp.clip(entries, min=-reach, max=reach).astype(kind)


def setup_inputs(seed: int = 0) -> dict:
    key_list = jax.random.split(jax.random.key(seed), 14)
    tokens = draw_tokens(jax.random.fold_in(key_list[13], 71), 0)
    spatial_queries = draw_spatial_queries(jax.random.fold_in(key_list[13], 71), 0)
    spatial_keys = draw_spatial_keys(jax.random.fold_in(key_list[13], 71), 0)
    spatial_values = gaussian(key_list[3], (CLIPS, FRAMES, POS, HH), 1.0, 6.0, ((0, 4), (1, 8)))
    spatial_proj = gaussian(key_list[4], (HH, D), HH ** -0.5, 0.1875, ((0, 8),))
    temporal_qkv = draw_temporal_qkv(jax.random.fold_in(key_list[13], 71), 0)
    temporal_proj = gaussian(key_list[6], (HH, D), HH ** -0.5, 0.1875, ((0, 8),))
    frame_mask = draw_frame_mask(jax.random.fold_in(key_list[13], 71), 0)
    expert_ids_keys = jax.random.split(jax.random.fold_in(key_list[8], 1), CLIPS * FRAMES * POS // POS)
    expert_ids_turns = jax.random.permutation(jax.random.fold_in(key_list[8], 3), CLIPS * FRAMES * POS // POS)
    expert_ids = jax.vmap(lambda own, number: deal_out(jax.random.fold_in(key_list[8], 2), own, number, POS, EXPERTS, TOP, CAP, 2))(expert_ids_keys, expert_ids_turns).reshape((CLIPS, FRAMES, POS, TOP))
    gate_values = jnp.clip(0.2 + 0.8 * jax.random.uniform(key_list[9], (CLIPS, FRAMES, POS, TOP), jnp.float32) ** block_levels(key_list[9], (CLIPS, FRAMES, POS, TOP), ((0, 4), (1, 8)), -0.2, 0.2), 0.2, 1.0)
    expert_gate = gaussian(key_list[10], (EXPERTS, D, FF), D ** -0.5, 0.125, ((0, 32),))
    expert_up = gaussian(key_list[11], (EXPERTS, D, FF), D ** -0.5, 0.125, ((0, 32),))
    expert_down = gaussian(key_list[12], (EXPERTS, FF, D), FF ** -0.5, 0.15625, ((0, 32),))
    return {"tokens": tokens, "spatial_queries": spatial_queries, "spatial_keys": spatial_keys, "spatial_values": spatial_values, "spatial_proj": spatial_proj, "temporal_qkv": temporal_qkv, "temporal_proj": temporal_proj, "frame_mask": frame_mask, "expert_ids": expert_ids, "gate_values": gate_values, "expert_gate": expert_gate, "expert_up": expert_up, "expert_down": expert_down}


EPS = 1e-06
MASKED = -1e+30

def rms_normed(values):
    wide = values.astype(jnp.float32)
    inverse = lax.rsqrt(lax.optimization_barrier(jnp.mean(wide * wide, axis=-1, keepdims=True)) + EPS)
    return (wide * inverse).astype(jnp.bfloat16)

def normalize_rows(scores):
    row_max = lax.optimization_barrier(jnp.max(scores, axis=-1, keepdims=True))
    exp_terms = jnp.exp(scores - row_max)
    return (exp_terms / lax.optimization_barrier(jnp.sum(exp_terms, axis=-1, keepdims=True))).astype(jnp.bfloat16)

def spatial_clip(triple):
    queries, keys, values = triple
    score_scale = 1.0 / math.sqrt(HD)
    query_heads = queries.astype(jnp.float32).reshape(FRAMES, POS, HEADS, HD)
    key_heads = keys.astype(jnp.float32).reshape(FRAMES, POS, HEADS, HD)
    value_heads = values.astype(jnp.float32).reshape(FRAMES, POS, HEADS, HD)
    scores = jnp.einsum('fqhd,fkhd->fhqk', query_heads, key_heads) * score_scale
    weights = normalize_rows(scores)
    mixed = jnp.einsum('fhqk,fkhd->fqhd', weights.astype(jnp.float32), value_heads)
    return mixed.astype(jnp.bfloat16).reshape(FRAMES, POS, HEADS * HD)

def reference(tokens, spatial_queries, spatial_keys, spatial_values, spatial_proj, temporal_qkv, temporal_proj, frame_mask, expert_ids, gate_values, expert_gate, expert_up, expert_down):
    score_scale = 1.0 / math.sqrt(HD)
    spatial_mixed = lax.map(spatial_clip, (spatial_queries, spatial_keys, spatial_values))
    spatial_update = jnp.dot(spatial_mixed.reshape(-1, HEADS * HD), spatial_proj, preferred_element_type=jnp.float32)
    first = (tokens.reshape(-1, D).astype(jnp.float32) + spatial_update).astype(jnp.bfloat16)
    normed = rms_normed(first)
    triple = jnp.dot(normed, temporal_qkv, preferred_element_type=jnp.float32).astype(jnp.bfloat16)
    triple = triple.reshape(CLIPS, FRAMES, POS, 3, HEADS, HD).astype(jnp.float32)
    scores = jnp.einsum('ciphd,cjphd->cphij', triple[:, :, :, 0], triple[:, :, :, 1]) * score_scale
    allowed = (frame_mask == 1)[:, None, None, :, :]
    weights = normalize_rows(jnp.where(allowed, scores, MASKED))
    temporal_mixed = jnp.einsum('cphij,cjphd->ciphd', weights.astype(jnp.float32), triple[:, :, :, 2])
    temporal_mixed = temporal_mixed.astype(jnp.bfloat16).reshape(-1, HEADS * HD)
    temporal_update = jnp.dot(temporal_mixed, temporal_proj, preferred_element_type=jnp.float32).astype(jnp.bfloat16)
    second = (first.astype(jnp.float32) + temporal_update.astype(jnp.float32)).astype(jnp.bfloat16)
    routed = rms_normed(second)
    pair_ids = expert_ids.reshape(-1).astype(jnp.int32)
    pair_total = pair_ids.shape[0]
    ordering = jnp.argsort(pair_ids, stable=True).astype(jnp.int32)
    sorted_ids = pair_ids[ordering]
    counts = lax.optimization_barrier(jnp.sum((pair_ids[:, None] == jnp.arange(EXPERTS, dtype=jnp.int32)[None, :]).astype(jnp.int32), axis=0))
    starts = (jnp.cumsum(counts) - counts).astype(jnp.int32)
    rank_sorted = (jnp.arange(pair_total, dtype=jnp.int32) - starts[sorted_ids]).astype(jnp.int32)
    slot_table = jnp.full((EXPERTS, EXPERTS * CAP), -1, jnp.int32).at[sorted_ids, rank_sorted].set(ordering)
    rank_pair = jnp.zeros((pair_total,), jnp.int32).at[ordering].set(rank_sorted)

    def one_expert(pieces):
        pair_index, gate_rows, up_rows, down_rows = pieces
        present = pair_index >= 0
        token_index = (jnp.maximum(pair_index, 0) // TOP).astype(jnp.int32)
        token_rows = jnp.where(present[:, None], routed[token_index], jnp.zeros((), jnp.bfloat16))
        gate_part = jnp.dot(token_rows, gate_rows, preferred_element_type=jnp.float32)
        up_part = jnp.dot(token_rows, up_rows, preferred_element_type=jnp.float32)
        hidden = (jax.nn.silu(gate_part) * up_part).astype(jnp.bfloat16)
        return jnp.dot(hidden, down_rows, preferred_element_type=jnp.float32).astype(jnp.bfloat16)
    answers = lax.map(one_expert, (slot_table, expert_gate, expert_up, expert_down))
    pair_answers = answers[pair_ids, rank_pair].astype(jnp.float32).reshape(-1, TOP, D)
    expert_mix = lax.optimization_barrier(jnp.sum(pair_answers * gate_values.reshape(-1, TOP, 1), axis=1))
    layer_out = (second.astype(jnp.float32) + expert_mix).astype(jnp.bfloat16)
    return layer_out.reshape(CLIPS, FRAMES, POS, D)
```

```python
import functools
import math

import jax
import jax.numpy as jnp
from jax import lax
from jax.experimental import pallas as pl
from jax.experimental.pallas import tpu as pltpu
from jax.sharding import PartitionSpec as P

HEADS = 8
HD = 128
TOP = 2


EPS = 1e-06
MASKED = -1e30


def rms_normed(values):
    wide = values.astype(jnp.float32)
    inverse = lax.rsqrt(jnp.mean(wide * wide, axis=-1, keepdims=True) + EPS)
    return (wide * inverse).astype(jnp.bfloat16)


def normalize_rows(scores):
    row_max = jnp.max(scores, axis=-1, keepdims=True)
    exp_terms = jnp.exp(scores - row_max)
    return (exp_terms / jnp.sum(exp_terms, axis=-1, keepdims=True)).astype(jnp.bfloat16)


def add_columns(left_side, piece):
    return jnp.dot(left_side, piece, preferred_element_type=jnp.float32)


def spatial_mix(queries, keys, values):
    positions = queries.shape[0]
    score_scale = 1.0 / math.sqrt(HD)
    query_heads = queries.reshape(positions, HEADS, HD)
    key_heads = keys.reshape(positions, HEADS, HD)
    value_heads = values.reshape(positions, HEADS, HD)
    scores = (
        jnp.einsum("qhd,khd->hqk", query_heads, key_heads, preferred_element_type=jnp.float32)
        * score_scale
    )
    weights = normalize_rows(scores)
    mixed = jnp.einsum("hqk,khd->qhd", weights, value_heads, preferred_element_type=jnp.float32)
    return mixed.astype(jnp.bfloat16).reshape(positions, HEADS * HD)


def temporal_mix(queries, keys, values, allowed):
    frames, positions = (queries.shape[0], queries.shape[1])
    score_scale = 1.0 / math.sqrt(HD)
    query_heads = queries.reshape(frames, positions, HEADS, HD)
    key_heads = keys.reshape(frames, positions, HEADS, HD)
    value_heads = values.reshape(frames, positions, HEADS, HD)
    scores = (
        jnp.einsum("iphd,jphd->phij", query_heads, key_heads, preferred_element_type=jnp.float32)
        * score_scale
    )
    weights = normalize_rows(jnp.where(allowed[None, None, :, :], scores, MASKED))
    mixed = jnp.einsum("phij,jphd->iphd", weights, value_heads, preferred_element_type=jnp.float32)
    return mixed.astype(jnp.bfloat16).reshape(frames, positions, HEADS * HD)


def temporal_inputs(normed, qkv_rows):
    zero_start = jnp.zeros((normed.shape[0], qkv_rows.shape[1]), jnp.float32)

    def fold_rows(total, piece, start):
        return add_columns(normed, piece)

    return fold_rows(
        zero_start, lax.all_gather(qkv_rows, "tm", axis=0, tiled=True), jnp.int32(0)
    ).astype(jnp.bfloat16)


def temporal_output(mixed, proj_rows):
    zero_start = jnp.zeros((mixed.shape[0], proj_rows.shape[1]), jnp.float32)

    def fold_rows(total, piece, start):
        return add_columns(mixed, piece)

    return fold_rows(
        zero_start, lax.all_gather(proj_rows, "tm", axis=0, tiled=True), jnp.int32(0)
    ).astype(jnp.bfloat16)


LINK = pl.DeviceIdType.MESH
VMEM_BYTES = 60 * 1024 * 1024


def column_chunks(width):
    return 4 if width % 512 == 0 else 1


def greet(neighbours_line, plane_count):
    z = lax.axis_index("clip")
    me = lax.axis_index("tm")
    barrier = pltpu.get_barrier_semaphore()
    for step in range(1, plane_count):
        pl.semaphore_signal(
            barrier,
            inc=1,
            device_id={"tm": lax.rem(me + step, plane_count)},
            device_id_type=LINK,
        )

    @pl.when(z > 0)
    def _():
        pl.semaphore_signal(barrier, inc=1, device_id={"clip": z - 1}, device_id_type=LINK)

    @pl.when(z < neighbours_line - 1)
    def _():
        pl.semaphore_signal(barrier, inc=1, device_id={"clip": z + 1}, device_id_type=LINK)

    ends = (z == 0) | (z == neighbours_line - 1)

    @pl.when(ends)
    def _():
        pl.semaphore_wait(barrier, plane_count)

    @pl.when(jnp.logical_not(ends))
    def _():
        pl.semaphore_wait(barrier, plane_count + 1)


def dispatch_kernel(
    n, m, chunks, x_ref, pick_ref, out_ref, frames, stage, zsend, zrecv, xsend, xrecv, own_sem, loc
):
    z = lax.axis_index("clip")
    me = lax.axis_index("tm")
    width = x_ref.shape[1]
    cap = stage.shape[2]
    w = width // chunks
    first_copy = pltpu.make_async_copy(x_ref, frames.at[z], own_sem)
    first_copy.start()
    greet(n, m)
    first_copy.wait()

    def columns(c):
        return pl.ds(pl.multiple_of(c * w, w), w)

    def line_copy(to, f, s, c, way):
        return pltpu.make_async_remote_copy(
            src_ref=frames.at[f, :, columns(c)],
            dst_ref=frames.at[f, :, columns(c)],
            send_sem=zsend.at[way, s, c],
            recv_sem=zrecv.at[f, c],
            device_id={"clip": to},
            device_id_type=LINK,
        )

    def spread(f, c):
        rows = jnp.dot(
            pick_ref[f], frames[f, :, columns(c)], preferred_element_type=jnp.float32
        )
        for t in range(m):
            stage[f, t, :, columns(c)] = rows[t * cap : (t + 1) * cap].astype(jnp.bfloat16)
        for t in range(1, m):
            to = lax.rem(me + t, m)
            pltpu.make_async_remote_copy(
                src_ref=stage.at[f, to, :, columns(c)],
                dst_ref=out_ref.at[me, f, :, columns(c)],
                send_sem=xsend.at[t],
                recv_sem=xrecv.at[t],
                device_id={"tm": to},
                device_id_type=LINK,
            ).start()
        pltpu.make_async_copy(
            stage.at[f, me, :, columns(c)], out_ref.at[me, f, :, columns(c)], loc
        ).start()

    def step(i, carry):
        s = i // chunks
        c = lax.rem(i, chunks)
        for way in (0, 1):
            f = z - s if way == 0 else z + s
            to = z + 1 if way == 0 else z - 1
            here = f >= 0 if way == 0 else f <= n - 1
            onward = z < n - 1 if way == 0 else z > 0

            @pl.when(here & (s > 0))
            def _(f=f, c=c, s=s, to=to, way=way):
                line_copy(to, f, s, c, way).wait_recv()

            @pl.when(here & onward)
            def _(f=f, c=c, s=s, to=to, way=way):
                line_copy(to, f, s, c, way).start()

        for way in (0, 1):
            f = z - s if way == 0 else z + s
            here = f >= 0 if way == 0 else (f <= n - 1) & (s > 0)

            @pl.when(here)
            def _(f=f, c=c):
                spread(f, c)

        return carry

    lax.fori_loop(0, n * chunks, step, 0)

    def finish(i, carry):
        s = i // chunks
        c = lax.rem(i, chunks)
        for way in (0, 1):
            f = z - s if way == 0 else z + s
            to = z + 1 if way == 0 else z - 1
            here = f >= 0 if way == 0 else f <= n - 1
            onward = z < n - 1 if way == 0 else z > 0

            @pl.when(here & onward)
            def _(f=f, c=c, s=s, to=to, way=way):
                line_copy(to, f, s, c, way).wait_send()

        return carry

    lax.fori_loop(0, n * chunks, finish, 0)
    for t in range(1, m):
        to = lax.rem(me + t, m)
        whole = pltpu.make_async_remote_copy(
            src_ref=stage.at[:, to],
            dst_ref=out_ref.at[lax.rem(me + m - t, m)],
            send_sem=xsend.at[t],
            recv_sem=xrecv.at[t],
            device_id={"tm": to},
            device_id_type=LINK,
        )
        whole.wait_send()
        whole.wait_recv()
    pltpu.make_async_copy(stage.at[:, me], out_ref.at[me], loc).wait()


def dispatch(routed, pick, cap):
    n, m = lax.axis_size("clip"), lax.axis_size("tm")
    rows, width = routed.shape
    chunks = column_chunks(width)
    return pl.pallas_call(
        functools.partial(dispatch_kernel, n, m, chunks),
        out_shape=jax.ShapeDtypeStruct((m, n, cap, width), jnp.bfloat16),
        in_specs=[pl.BlockSpec(memory_space=pl.ANY), pl.BlockSpec(memory_space=pltpu.VMEM)],
        out_specs=pl.BlockSpec(memory_space=pltpu.VMEM),
        scratch_shapes=[
            pltpu.VMEM((n, rows, width), jnp.bfloat16),
            pltpu.VMEM((n, m, cap, width), jnp.bfloat16),
            pltpu.SemaphoreType.DMA((2, n, chunks)),
            pltpu.SemaphoreType.DMA((n, chunks)),
            pltpu.SemaphoreType.DMA((m,)),
            pltpu.SemaphoreType.DMA((m,)),
            pltpu.SemaphoreType.DMA,
            pltpu.SemaphoreType.DMA,
        ],
        compiler_params=pltpu.CompilerParams(
            collective_id=1, has_side_effects=True, vmem_limit_bytes=VMEM_BYTES
        ),
    )(routed, pick)


def combine_kernel(
    n, m, chunks, ans_ref, mix_ref, base_ref, out_ref, got, zin, zout, total, zsend, zrecv, xsend, xrecv
):
    z = lax.axis_index("clip")
    me = lax.axis_index("tm")
    width = base_ref.shape[1]
    cap = got.shape[2]
    w = width // chunks
    greet(n, m)

    def columns(c):
        return pl.ds(pl.multiple_of(c * w, w), w)

    def send_plane(f, c):
        for t in range(1, m):
            to = lax.rem(me + t, m)
            pltpu.make_async_remote_copy(
                src_ref=ans_ref.at[to, f, :, columns(c)],
                dst_ref=got.at[me, f, :, columns(c)],
                send_sem=xsend.at[t],
                recv_sem=xrecv.at[f, c],
                device_id={"tm": to},
                device_id_type=LINK,
            ).start()
        pltpu.make_async_copy(
            ans_ref.at[me, f, :, columns(c)], got.at[me, f, :, columns(c)], xrecv.at[f, c]
        ).start()

    def ordered(act):
        def step(i, carry):
            s = i // chunks
            c = lax.rem(i, chunks)
            for way in (0, 1):
                f = n - 1 - s if way == 0 else s

                @pl.when(f > z if way == 0 else f < z)
                def _(f=f, c=c, way=way):
                    act(f, c, way)

            return carry

        lax.fori_loop(0, n * chunks, step, 0)

        def last(c, carry):
            act(z, c, 2)
            return carry

        lax.fori_loop(0, chunks, last, 0)

    ordered(lambda f, c, way: send_plane(f, c))

    def line_copy(f, c, way):
        return pltpu.make_async_remote_copy(
            src_ref=zout.at[f, :, columns(c)],
            dst_ref=zin.at[f + 1 - way, :, columns(c)],
            send_sem=zsend.at[f, c],
            recv_sem=zrecv.at[f + 1 - way, c],
            device_id={"clip": z + 1 - 2 * way},
            device_id_type=LINK,
        )

    def add_line(f, c, way):
        line_copy(f, c, way).wait_recv()
        total[...] += zin[f + 1 - way, :, columns(c)].astype(jnp.float32)

    def work(f, c, way):
        pltpu.make_async_copy(
            got.at[:, f, :, columns(c)], got.at[:, f, :, columns(c)], xrecv.at[f, c]
        ).wait()
        if cap % 16 == 0:
            slots = got[:, f, :, columns(c)].reshape(m * cap, w)
        else:
            slots = jnp.concatenate(
                [got[t, f, :, columns(c)].astype(jnp.float32) for t in range(m)], axis=0
            ).astype(jnp.bfloat16)
        total[...] = jnp.dot(mix_ref[f], slots, preferred_element_type=jnp.float32)
        if way != 1:

            @pl.when(z > 0)
            def _():
                add_line(f, c, 0)

        if way != 0:

            @pl.when(z < n - 1)
            def _():
                add_line(f, c, 1)

        if way == 2:
            out_ref[:, columns(c)] = (
                base_ref[:, columns(c)].astype(jnp.float32) + total[...]
            ).astype(jnp.bfloat16)
        else:
            zout[f, :, columns(c)] = total[...].astype(jnp.bfloat16)
            line_copy(f, c, way).start()

    ordered(work)

    def finish(f, c, way):
        if way != 2:
            line_copy(f, c, way).wait_send()

    ordered(finish)
    for t in range(1, m):
        to = lax.rem(me + t, m)
        pltpu.make_async_remote_copy(
            src_ref=ans_ref.at[to],
            dst_ref=got.at[me],
            send_sem=xsend.at[t],
            recv_sem=xrecv.at[0, 0],
            device_id={"tm": to},
            device_id_type=LINK,
        ).wait_send()


def combine(answers, mix, base):
    n, m = lax.axis_size("clip"), lax.axis_size("tm")
    rows, width = base.shape
    cap = answers.shape[2]
    chunks = column_chunks(width)
    vmem = pl.BlockSpec(memory_space=pltpu.VMEM)
    return pl.pallas_call(
        functools.partial(combine_kernel, n, m, chunks),
        out_shape=jax.ShapeDtypeStruct((rows, width), jnp.bfloat16),
        in_specs=[pl.BlockSpec(memory_space=pl.ANY), vmem, vmem],
        out_specs=vmem,
        scratch_shapes=[
            pltpu.VMEM((m, n, cap, width), jnp.bfloat16),
            pltpu.VMEM((n + 1, rows, width), jnp.bfloat16),
            pltpu.VMEM((n, rows, width), jnp.bfloat16),
            pltpu.VMEM((rows, width // chunks), jnp.float32),
            pltpu.SemaphoreType.DMA((n, chunks)),
            pltpu.SemaphoreType.DMA((n + 1, chunks)),
            pltpu.SemaphoreType.DMA((m,)),
            pltpu.SemaphoreType.DMA((n, chunks)),
        ],
        compiler_params=pltpu.CompilerParams(
            collective_id=2, has_side_effects=True, vmem_limit_bytes=VMEM_BYTES
        ),
    )(answers, mix, base)


def shards(
    tokens,
    spatial_queries,
    spatial_keys,
    spatial_values,
    spatial_proj,
    temporal_qkv,
    temporal_proj,
    frame_mask,
    expert_ids,
    gate_values,
    expert_gate,
    expert_up,
    expert_down,
):
    model_width = tokens.shape[3]
    positions = tokens.shape[2]
    tm_count = lax.axis_size("tm")
    clip_count = lax.axis_size("clip")
    experts = clip_count * tm_count
    per_block = positions // tm_count
    resident = tokens.reshape(positions, model_width)
    attended_space = spatial_mix(
        spatial_queries.reshape(positions, -1),
        spatial_keys.reshape(positions, -1),
        spatial_values.reshape(positions, -1),
    )
    spatial_update = add_columns(
        attended_space, lax.all_gather(spatial_proj, "tm", axis=0, tiled=True)
    )
    first = (resident.astype(jnp.float32) + spatial_update).astype(jnp.bfloat16)
    normed = rms_normed(first)
    allowed = frame_mask[0] == 1
    by_position = lax.all_to_all(
        normed.reshape(tm_count, per_block, model_width),
        "tm",
        split_axis=0,
        concat_axis=0,
        tiled=True,
    )
    frames = by_position.shape[0]
    projected = temporal_inputs(by_position.reshape(frames * per_block, model_width), temporal_qkv)
    head_width = projected.shape[1] // 3
    triple = projected.reshape(frames, per_block, 3 * head_width)
    attended_time = temporal_mix(
        triple[:, :, :head_width],
        triple[:, :, head_width : 2 * head_width],
        triple[:, :, 2 * head_width :],
        allowed,
    )
    update_rows = temporal_output(
        attended_time.reshape(frames * per_block, head_width), temporal_proj
    )
    returned = lax.all_to_all(
        update_rows.reshape(frames, per_block, model_width),
        "tm",
        split_axis=0,
        concat_axis=0,
        tiled=True,
    )
    temporal_update = returned.reshape(positions, model_width)
    second = (first.astype(jnp.float32) + temporal_update.astype(jnp.float32)).astype(jnp.bfloat16)
    routed = rms_normed(second)
    capacity = 2 * TOP * positions // experts
    pair_ids = expert_ids.reshape(positions * TOP)
    chosen = (pair_ids[:, None] == jnp.arange(experts, dtype=jnp.int32)[None, :]).astype(jnp.int32)
    earlier = jnp.cumsum(chosen, axis=0) - chosen
    pair_rank = jnp.sum(earlier * chosen, axis=1)
    pair_slot = pair_ids * capacity + pair_rank
    told = jnp.stack([pair_slot.astype(jnp.float32), gate_values.reshape(positions * TOP)])
    told = lax.all_gather(told, "clip", axis=0)
    plane_slots = tm_count * capacity
    slots_here = told[:, 0].astype(jnp.int32) - lax.axis_index("clip") * plane_slots
    slots_here = slots_here.reshape(clip_count, positions, TOP)
    gates_here = told[:, 1].reshape(clip_count, positions, TOP)
    slot_index = jnp.arange(plane_slots, dtype=jnp.int32)
    pick = jnp.zeros((clip_count, plane_slots, positions), jnp.bool_)
    mix = jnp.zeros((clip_count, positions, plane_slots), jnp.float32)
    for k in range(TOP):
        pick = pick | (slots_here[:, None, :, k] == slot_index[None, :, None])
        mix = mix + jnp.where(
            slots_here[:, :, k, None] == slot_index[None, None, :], gates_here[:, :, k, None], 0.0
        )
    received = dispatch(routed, pick.astype(jnp.bfloat16), capacity)
    flat_rows = received.reshape(-1, model_width)
    gate_part = jnp.dot(flat_rows, expert_gate[0], preferred_element_type=jnp.float32)
    up_part = jnp.dot(flat_rows, expert_up[0], preferred_element_type=jnp.float32)
    hidden = (jax.nn.silu(gate_part) * up_part).astype(jnp.bfloat16)
    answer = jnp.dot(hidden, expert_down[0], preferred_element_type=jnp.float32).astype(
        jnp.bfloat16
    )
    layer_out = combine(answer.reshape(received.shape), mix.astype(jnp.bfloat16), second)
    return layer_out.reshape(tokens.shape)


def solution(mesh):
    placed = (
        P("clip", "tm", None, None),
        P("clip", "tm", None, None),
        P("clip", "tm", None, None),
        P("clip", "tm", None, None),
        P("tm", None),
        P("tm", None),
        P("tm", None),
        P("clip", None, None),
        P("clip", "tm", None, None),
        P("clip", "tm", None, None),
        P(("clip", "tm"), None, None),
        P(("clip", "tm"), None, None),
        P(("clip", "tm"), None, None),
    )
    return jax.shard_map(
        shards, mesh=mesh, in_specs=placed, out_specs=P("clip", "tm", None, None), check_vma=False
    )
```
